32 devices in a mesh: tm: 8 (over z, y), node: 4 (over x, core).
Axes of the slice: x: 2, y: 2, z: 4, core: 2. Of those that a mesh axis runs over, the one named last changes fastest.
Arguments:
- slice_starts: float32 [8, 32, 16384], P('tm'), may hold values from -1 to 1
- coupling: float32 [32, 16384], replicated, may hold values from 0.03 to 0.25
Outputs:
- node_values: float32 [8, 4, 32, 16384], P('tm', 'node')
- residual_log: float32 [3, 32], replicated
The draws below stay inside these ranges and needn't reach their ends.
All inputs are finite; a program needn't handle non-finite values.
Results may differ from the reference program's by a relative error of at most 0.0001.
Values sent between devices are 32-bit elements.
No kernel may reach another device: no remote copies, remote signals or barrier semaphores. Data moves between devices by JAX's collectives and lax.ppermute only.
A program may use at most 128 MiB of HBM per device.

```python
import math
import jax
import jax.numpy as jnp
from jax import lax

X = 16384
SYS = 32
M = 4
SWEEPS = 3
NEWTON = 2
SLICES = 8


def block_scale(stream_key, shape, pieces, least, top_value):
    level, own = 1.0, jax.random.fold_in(stream_key, 6)
    for position, shards_of in pieces:
        draws = jnp.exp(jax.random.uniform(jax.random.fold_in(own, position), (shards_of,), jnp.float32, least / len(pieces), top_value / len(pieces)))
        level = level * jnp.repeat(draws, shape[position] // shards_of).reshape([-1 if axis == position else 1 for axis in range(len(shape))])
    return level


def setup_inputs(seed: int = 0) -> dict:
    key_of = jax.random.split(jax.random.key(seed), 3)
    return {
        "slice_starts": jnp.clip(jax.random.uniform(key_of[0], (SLICES, SYS, X), jnp.float32, -1.0, 1.0) * block_scale(key_of[0], (SLICES, SYS, X), ((0, 8),), -0.4, 0.0), -1.0, 1.0),
        "coupling": jnp.clip(jnp.exp(jax.random.uniform(key_of[1], (SYS, X), jnp.float32, math.log(0.03), math.log(0.25))), 0.03, 0.25),
    }


time_step = 0.5
log_floor = 0.05


def legendre_gap(point, node_count):
    before = 1.0
    current = point
    for degree in range(1, node_count):
        following = ((2 * degree + 1) * point * current - degree * before) / (degree + 1)
        before = current
        current = following
    return current - before


def collocation(node_count):
    points = []
    samples = 4000
    for sample_index in range(samples - 1):
        lower_end = -1.0 + 2.0 * sample_index / samples
        upper_end = -1.0 + 2.0 * (sample_index + 1) / samples
        lower_value = legendre_gap(lower_end, node_count)
        upper_value = legendre_gap(upper_end, node_count)
        if lower_value * upper_value < 0.0:
            for halving in range(80):
                middle = 0.5 * (lower_end + upper_end)
                middle_value = legendre_gap(middle, node_count)
                if lower_value * middle_value <= 0.0:
                    upper_end = middle
                else:
                    lower_end = middle
                    lower_value = middle_value
            points.append(0.5 * (lower_end + upper_end))
    points.append(1.0)
    node_times = [(point + 1.0) / 2.0 for point in points]
    matrix = [[0.0] * node_count for row_index in range(node_count)]
    for column in range(node_count):
        coeffs = [1.0]
        for other in range(node_count):
            if other != column:
                scale = node_times[column] - node_times[other]
                shifted = [0.0] + coeffs
                scaled = [value * node_times[other] for value in coeffs] + [0.0]
                coeffs = [(shifted[power] - scaled[power]) / scale for power in range(len(shifted))]
        for row_index in range(node_count):
            upper_time = node_times[row_index]
            matrix[row_index][column] = sum(coeffs[power] * upper_time ** (power + 1) / (power + 1) for power in range(len(coeffs)))
    return node_times, matrix


def operator_term(field_values, coupling):
    right_side = jnp.roll(field_values, -1, axis=-1)
    left_side = jnp.roll(field_values, 1, axis=-1)
    left_coupling = jnp.roll(coupling, 1, axis=-1)
    cubic = field_values * field_values * field_values
    return coupling * (right_side - field_values) - left_coupling * (field_values - left_side) + field_values - cubic


def reference(slice_starts, coupling):
    node_times, matrix = collocation(M)
    weights = jnp.asarray(matrix, jnp.float32)
    diag_weights = jnp.asarray([time_step * moment / M for moment in node_times], jnp.float32)
    implicit = diag_weights[None, :, None, None]
    node_state = jnp.broadcast_to(slice_starts[:, None], (SLICES, M, SYS, X))
    end_values = slice_starts
    residual_list = []
    for sweep_index in range(SWEEPS):
        starts = jnp.concatenate([slice_starts[:1], end_values[:-1]], axis=0)
        forcing = operator_term(node_state, coupling)
        quadrature = jnp.einsum("mj,pjsx->pmsx", weights, forcing, precision=lax.Precision.HIGHEST)
        base = starts[:, None] + time_step * quadrature
        defect = base - node_state
        mean_square = jnp.sum(defect * defect, axis=(0, 1, 3)) / (SLICES * M * X)
        residual_list.append(jnp.log(log_floor + mean_square))
        target = base - implicit * (node_state - node_state * node_state * node_state)
        iterate = node_state
        for newton_step in range(NEWTON):
            cubic = iterate * iterate * iterate
            derivative = 1.0 - implicit + 3.0 * implicit * iterate * iterate
            iterate = iterate - (iterate - implicit * (iterate - cubic) - target) / derivative
        node_state = iterate
        end_values = node_state[:, M - 1]
    return node_state, jnp.stack(residual_list)
```

```python
import functools

import jax
import jax.numpy as jnp
from jax import lax
from jax.experimental import pallas as pl
from jax.experimental.pallas import tpu as pltpu
from jax.sharding import PartitionSpec as P

M = 4
SWEEPS = 3
NEWTON = 2
LANES = 128
CHUNKS = 2
WIDTH = 512

time_step = 0.5
log_floor = 0.05


def legendre_gap(point, node_count):
    before = 1.0
    current = point
    for degree in range(1, node_count):
        following = ((2 * degree + 1) * point * current - degree * before) / (degree + 1)
        before = current
        current = following
    return current - before


def collocation(node_count):
    points = []
    samples = 4000
    for sample_index in range(samples - 1):
        lower_end = -1.0 + 2.0 * sample_index / samples
        upper_end = -1.0 + 2.0 * (sample_index + 1) / samples
        lower_value = legendre_gap(lower_end, node_count)
        upper_value = legendre_gap(upper_end, node_count)
        if lower_value * upper_value < 0.0:
            for halving in range(80):
                middle = 0.5 * (lower_end + upper_end)
                middle_value = legendre_gap(middle, node_count)
                if lower_value * middle_value <= 0.0:
                    upper_end = middle
                else:
                    lower_end = middle
                    lower_value = middle_value
            points.append(0.5 * (lower_end + upper_end))
    points.append(1.0)
    node_times = [(point + 1.0) / 2.0 for point in points]
    matrix = [[0.0] * node_count for row_index in range(node_count)]
    for column in range(node_count):
        coeffs = [1.0]
        for other in range(node_count):
            if other != column:
                scale = node_times[column] - node_times[other]
                shifted = [0.0] + coeffs
                scaled = [value * node_times[other] for value in coeffs] + [0.0]
                coeffs = [(shifted[power] - scaled[power]) / scale for power in range(len(shifted))]
        for row_index in range(node_count):
            upper_time = node_times[row_index]
            matrix[row_index][column] = sum(
                (
                    coeffs[power] * upper_time ** (power + 1) / (power + 1)
                    for power in range(len(coeffs))
                )
            )
    return (node_times, matrix)


NODE_TIMES, MATRIX = collocation(M)
LAST = M - 1
WEIGHTS = [[time_step * entry for entry in row] for row in MATRIX]
ROW_SUMS = [time_step * moment for moment in NODE_TIMES]
IMPLICIT = [time_step * moment / M for moment in NODE_TIMES]


def newton_steps(base, value, square, weight):
    rest = base - weight * value
    tripled = square * (3.0 * weight)
    cubic = tripled * value
    target = rest + cubic * (1.0 / 3.0)
    value = (rest + cubic) / (tripled + (1.0 - weight))
    for newton_step in range(1, NEWTON):
        tripled = (value * value) * (3.0 * weight)
        numerator = target + (tripled * value) * (2.0 / 3.0)
        value = numerator / (tripled + (1.0 - weight))
    return value


def weighted(terms, row):
    total = terms[0] * row[0]
    for term, entry in zip(terms[1:], row[1:]):
        total = total + term * entry
    return total


def chunk_kernel(
    place, coupling, mine, partner, straight, crossed, far_same, far_other,
    out, residual,
    v_lo, v_hi, v_h1, v_h2, v_h3, e_h2, e_h1, u_h1, u_lo, u_hi, w_lo, w_hi,
):
    side = place[0]
    node = place[1]
    first = place[2] == 0
    second = place[2] == 1
    length = coupling.shape[1]
    core = length - 2 * LANES
    width = min(WIDTH, core)

    def field(read, offset, size, left_edge, right_edge):
        value = read(pl.ds(offset, size))
        before = value[:, :LANES] if left_edge else read(pl.ds(offset - LANES, LANES))
        after = value[:, size - LANES :] if right_edge else read(pl.ds(offset + size, LANES))
        whole = jnp.concatenate([before, value, after], axis=1)
        left_coupling = (
            coupling[:, pl.ds(offset, LANES)]
            if left_edge
            else coupling[:, pl.ds(offset - LANES, LANES)]
        )
        factor = jnp.concatenate([left_coupling, coupling[:, pl.ds(offset, size)]], axis=1)
        right = pltpu.roll(whole, size + 2 * LANES - 1, 1)[:, : size + LANES]
        flux = factor * (right - whole[:, : size + LANES])
        left = pltpu.roll(flux, 1, 1)[:, LANES:]
        square = value * value
        slope = (flux[:, LANES:] - left) + (value - value * square)
        return value, square, slope

    def squares(total, defect):
        pieces = defect * defect
        for piece in range(pieces.shape[1] // LANES):
            total = total + pieces[:, piece * LANES : (piece + 1) * LANES]
        return total

    def sweep(block, edges):
        zero = jnp.zeros((coupling.shape[0], LANES), jnp.float32)
        if edges:
            block(0, LANES, True, False, zero)
            block(length - LANES, LANES, False, True, zero)

        def step(index, total):
            offset = pl.multiple_of(LANES + index * width, LANES)
            return block(offset, width, False, False, total)

        return lax.fori_loop(0, core // width, step, zero)

    def pick(index, carry):
        span = pl.ds(pl.multiple_of(index * LANES, LANES), LANES)
        v_lo[:, span] = jnp.where(side == 0, mine[:, span], partner[:, span])
        v_hi[:, span] = jnp.where(side == 0, partner[:, span], mine[:, span])
        v_h1[:, span] = jnp.where(side == 0, crossed[:, span], straight[:, span])
        v_h2[:, span] = jnp.where(side == 0, straight[:, span], crossed[:, span])
        v_h3[:, span] = jnp.where(side == 0, far_other[:, span], far_same[:, span])
        return carry

    lax.fori_loop(0, length // LANES, pick, 0)

    def opening(start, value_ref, store, nodes):
        def block(offset, size, left_edge, right_edge, total):
            span = pl.ds(offset, size)
            value, square, slope = field(
                lambda at: value_ref[:, at], offset, size, left_edge, right_edge
            )
            origin = start(span)
            for index in nodes:
                base = origin + slope * ROW_SUMS[index]
                total = squares(total, base - value)
                store(index, span, newton_steps(base, value, square, IMPLICIT[index]))
            return total

        return sweep(block, True)

    def keep(ref):
        def store(index, span, value):
            ref[index, :, span] = value

        return store

    def keep_one(ref):
        def store(index, span, value):
            ref[:, span] = value

        return store

    def later(start, state, store, nodes, edges):
        def block(offset, size, left_edge, right_edge, total):
            span = pl.ds(offset, size)
            fields = [
                field(
                    functools.partial(lambda j, at: state[j, :, at], j),
                    offset, size, left_edge, right_edge,
                )
                for j in range(M)
            ]
            slopes = [entry[2] for entry in fields]
            origin = start(span)
            for index in nodes:
                value, square = fields[index][:2]
                base = origin + weighted(slopes, WEIGHTS[index])
                total = squares(total, base - value)
                store(index, span, newton_steps(base, value, square, IMPLICIT[index]))
            return total

        return sweep(block, edges)

    def emit(target):
        def store(index, span, value):
            at = pl.ds(span.start - LANES, span.size)
            out[target ^ side, index ^ node, :, at] = value

        return store

    every = range(M)
    opening(
        lambda s: jnp.where(second, v_h2[:, s], v_h3[:, s]), v_h2, keep_one(e_h2), [LAST]
    )
    opening(lambda s: v_h2[:, s], v_h1, keep(u_h1), every)
    sum_lo = opening(
        lambda s: jnp.where(first, v_lo[:, s], v_h1[:, s]), v_lo, keep(u_lo), every
    )
    sum_hi = opening(lambda s: v_lo[:, s], v_hi, keep(u_hi), every)
    residual[0] = sum_lo + sum_hi
    later(lambda s: e_h2[:, s], u_h1, keep_one(e_h1), [LAST], True)
    sum_lo = later(
        lambda s: jnp.where(first, v_lo[:, s], u_h1[LAST, :, s]), u_lo, keep(w_lo), every, True
    )
    sum_hi = later(lambda s: u_lo[LAST, :, s], u_hi, keep(w_hi), every, True)
    residual[1] = sum_lo + sum_hi
    sum_lo = later(
        lambda s: jnp.where(first, v_lo[:, s], e_h1[:, s]), w_lo, emit(0), every, False
    )
    sum_hi = later(lambda s: w_lo[LAST, :, s], w_hi, emit(1), every, False)
    residual[2] = sum_lo + sum_hi


def run_chunk(place, coupling, pieces):
    rows, length = coupling.shape
    core = length - 2 * LANES
    flat = pltpu.VMEM((rows, length), jnp.float32)
    deep = pltpu.VMEM((M, rows, length), jnp.float32)
    vmem = pl.BlockSpec(memory_space=pltpu.VMEM)
    return pl.pallas_call(
        chunk_kernel,
        out_shape=(
            jax.ShapeDtypeStruct((2, M, rows, core), jnp.float32),
            jax.ShapeDtypeStruct((SWEEPS, rows, LANES), jnp.float32),
        ),
        in_specs=[pl.BlockSpec(memory_space=pltpu.SMEM)] + [vmem] * (1 + len(pieces)),
        out_specs=(vmem, vmem),
        scratch_shapes=[flat] * 7 + [deep] * 5,
        cost_estimate=pl.CostEstimate(
            flops=1000 * rows * length, bytes_accessed=64 * rows * length, transcendentals=0
        ),
        name="sweeps",
    )(place, coupling, *pieces)


def gather_kernel(half, chunk, place, *refs):
    blocks, out, stage, load, save = refs[:-4], refs[-4], refs[-3], refs[-2], refs[-1]
    side = place[0]
    node = place[1]
    rows = blocks[0].shape[0]

    def copies(index):
        part, rest = index // (2 * M), index % (2 * M)
        flip, other = rest // M, rest % M
        column = (flip ^ side) * half + part * chunk
        target = out.at[
            pl.ds(pl.multiple_of((other ^ node) * rows, rows), rows),
            pl.ds(pl.multiple_of(column, LANES), chunk),
        ]
        return (
            pltpu.make_async_copy(blocks[index], stage.at[index], load.at[index]),
            pltpu.make_async_copy(stage.at[index], target, save.at[index]),
        )

    pairs = [copies(index) for index in range(len(blocks))]
    for fetch, write in pairs:
        fetch.start()
    for fetch, write in pairs:
        fetch.wait()
        write.start()
    for fetch, write in pairs:
        write.wait()


def gather_blocks(place, blocks, half, systems):
    rows, chunk = blocks[0].shape
    count = len(blocks)
    return pl.pallas_call(
        functools.partial(gather_kernel, half, chunk),
        out_shape=jax.ShapeDtypeStruct((systems, 2 * half), jnp.float32),
        in_specs=[pl.BlockSpec(memory_space=pltpu.SMEM)]
        + [pl.BlockSpec(memory_space=pl.ANY)] * count,
        out_specs=pl.BlockSpec(memory_space=pl.ANY),
        scratch_shapes=[
            pltpu.VMEM((count, rows, chunk), jnp.float32),
            pltpu.SemaphoreType.DMA((count,)),
            pltpu.SemaphoreType.DMA((count,)),
        ],
        cost_estimate=pl.CostEstimate(
            flops=count * rows * chunk, bytes_accessed=8 * count * rows * chunk, transcendentals=0
        ),
        name="assemble",
    )(place, *blocks)


def body(slice_starts, coupling):
    slices = lax.axis_size("tm")
    systems, cells = coupling.shape
    rows = systems // M
    half = cells // 2
    chunk = half // CHUNKS
    length = chunk + 2 * LANES
    slice_pos = lax.axis_index("tm")
    node_pos = lax.axis_index("node")
    side = slice_pos % 2
    place = jnp.stack([side, node_pos, slice_pos // 2]).astype(jnp.int32)

    def padded(field):
        mine = lax.dynamic_slice(field, (node_pos * rows, 0), (rows, cells))
        return jnp.concatenate([mine[:, cells - LANES :], mine, mine[:, :LANES]], axis=1)

    starts = padded(slice_starts[0])
    couplings = padded(coupling)

    def piece(field, which, index):
        return lax.dynamic_slice(field, (0, which * half + index * chunk), (rows, length))

    def moved(value, target):
        pairs = [(i, target(i)) for i in range(slices)]
        pairs = [(i, j) for i, j in pairs if j is not None and 0 <= j < slices]
        return lax.ppermute(value, "tm", pairs)

    received = []
    for index in range(CHUNKS):
        mine = piece(starts, side, index)
        other = piece(starts, 1 - side, index)
        received.append(
            (
                mine,
                moved(other, lambda i: i ^ 1),
                moved(mine, lambda i: i + 2),
                moved(other, lambda i: (i ^ 1) + 2),
                moved(mine, lambda i: i + 4 if i % 2 else None),
                moved(other, lambda i: i + 3 if i % 2 else None),
            )
        )
    blocks = []
    partial = jnp.zeros((SWEEPS, rows), jnp.float32)
    count = slices * M
    for index in range(CHUNKS):
        out, sums = run_chunk(place, piece(couplings, side, index), received[index])
        partial = partial + jnp.sum(sums, axis=2)
        for flip in range(2):
            for other in range(M):
                block = out[flip, other]
                step = flip * M + other
                if step:
                    pairs = [(i, i ^ step) for i in range(count)]
                    block = lax.ppermute(block, ("tm", "node"), pairs)
                blocks.append(block)
    result = gather_blocks(place, blocks, half, systems)

    flat = jnp.pad(partial.reshape(-1), (0, -(SWEEPS * rows) % LANES))
    shared = lax.all_to_all(
        jnp.broadcast_to(flat[None], (count, flat.shape[0])), ("tm", "node"), 0, 0
    )
    summed = jnp.sum(shared.reshape(slices, M, -1), axis=0)[:, : SWEEPS * rows]
    summed = summed.reshape(M, SWEEPS, rows).transpose(1, 0, 2).reshape(SWEEPS, systems)
    residual_log = jnp.log(log_floor + summed / (slices * M * cells))
    return (result[None, None], residual_log)


def solution(mesh):
    placed = (P("tm", None, None), P())
    return jax.shard_map(
        body,
        mesh=mesh,
        in_specs=placed,
        out_specs=(P("tm", "node", None, None), P()),
        check_vma=False,
    )
```

```python
import functools

import jax
import jax.numpy as jnp
from jax import lax
from jax.experimental import pallas as pl
from jax.experimental.pallas import tpu as pltpu
from jax.sharding import PartitionSpec as P


M = 4
SWEEPS = 3
NEWTON = 2
LANES = 128
CHUNKS = 2
GROUP = 17
LARGE_LIMIT = 24 * 1024 * 1024
SMALL_LIMIT = 8 * 1024 * 1024

time_step = 0.5
log_floor = 0.05


def legendre_gap(point, node_count):
    before = 1.0
    current = point
    for degree in range(1, node_count):
        following = ((2 * degree + 1) * point * current - degree * before) / (degree + 1)
        before = current
        current = following
    return current - before


def collocation(node_count):
    points = []
    samples = 4000
    for sample_index in range(samples - 1):
        lower_end = -1.0 + 2.0 * sample_index / samples
        upper_end = -1.0 + 2.0 * (sample_index + 1) / samples
        lower_value = legendre_gap(lower_end, node_count)
        upper_value = legendre_gap(upper_end, node_count)
        if lower_value * upper_value < 0.0:
            for _ in range(80):
                middle = 0.5 * (lower_end + upper_end)
                middle_value = legendre_gap(middle, node_count)
                if lower_value * middle_value <= 0.0:
                    upper_end = middle
                else:
                    lower_end = middle
                    lower_value = middle_value
            points.append(0.5 * (lower_end + upper_end))
    points.append(1.0)
    node_times = [(point + 1.0) / 2.0 for point in points]
    matrix = [[0.0] * node_count for _ in range(node_count)]
    for column in range(node_count):
        coeffs = [1.0]
        for other in range(node_count):
            if other != column:
                scale = node_times[column] - node_times[other]
                shifted = [0.0] + coeffs
                scaled = [value * node_times[other] for value in coeffs] + [0.0]
                coeffs = [(shifted[power] - scaled[power]) / scale for power in range(len(shifted))]
        for row_index in range(node_count):
            upper_time = node_times[row_index]
            matrix[row_index][column] = sum(
                (
                    coeffs[power] * upper_time ** (power + 1) / (power + 1)
                    for power in range(len(coeffs))
                )
            )
    return (node_times, matrix)


NODE_TIMES, MATRIX = collocation(M)
LAST = M - 1
WEIGHTS = [[time_step * entry for entry in row] for row in MATRIX]
ROW_SUMS = [time_step * moment for moment in NODE_TIMES]
IMPLICIT = [time_step * moment / M for moment in NODE_TIMES]


def newton_steps(base, value, square, weight):
    rest = base - weight * value
    tripled = square * (3.0 * weight)
    cubic = tripled * value
    target = rest + cubic * (1.0 / 3.0)
    value = (rest + cubic) / (tripled + (1.0 - weight))
    for _ in range(1, NEWTON):
        tripled = (value * value) * (3.0 * weight)
        numerator = target + (tripled * value) * (2.0 / 3.0)
        value = numerator / (tripled + (1.0 - weight))
    return value


def weighted(terms, row):
    total = terms[0] * row[0]
    for term, entry in zip(terms[1:], row[1:]):
        total = total + term * entry
    return total


def group_of(count):
    return max(size for size in range(1, GROUP + 1) if count % size == 0)


def lanes_at(offset):
    return pl.ds(pl.multiple_of(offset, LANES), LANES)


def tracks(source, target, row, column, cells, core, sem):
    rows = target.shape[0]
    part = source.at[pl.ds(pl.multiple_of(row, rows), rows), :]
    before = pl.multiple_of(lax.rem(column + (cells - LANES), cells), LANES)
    after = pl.multiple_of(lax.rem(column + core, cells), LANES)
    middle = pl.multiple_of(column, LANES)
    return [
        pltpu.make_async_copy(
            part.at[:, pl.ds(before, LANES)], target.at[:, pl.ds(0, LANES)], sem.at[0]
        ),
        pltpu.make_async_copy(
            part.at[:, pl.ds(middle, core)], target.at[:, pl.ds(LANES, core)], sem.at[1]
        ),
        pltpu.make_async_copy(
            part.at[:, pl.ds(after, LANES)],
            target.at[:, pl.ds(LANES + core, LANES)],
            sem.at[2],
        ),
    ]


def place():
    position = lax.axis_index("tm")
    return lax.rem(position, 2), lax.div(position, 2), lax.axis_index("node")


def split_kernel(starts, couplings, mine, other, near, sems):
    side, _, node = place()
    rows, length = mine.shape
    cells = starts.shape[1]
    core = length - 2 * LANES
    copies = []
    for slot, (source, target, which) in enumerate(
        ((starts, mine, side), (starts, other, 1 - side), (couplings, near, side))
    ):
        copies += tracks(source, target, node * rows, which * core, cells, core, sems.at[slot])
    for copy in copies:
        copy.start()
    for copy in copies:
        copy.wait()


def split_starts(starts, couplings, rows, length):
    return pl.pallas_call(
        split_kernel,
        out_shape=[jax.ShapeDtypeStruct((rows, length), jnp.float32)] * 3,
        in_specs=[pl.BlockSpec(memory_space=pltpu.HBM)] * 2,
        out_specs=[pl.BlockSpec(memory_space=pltpu.VMEM)] * 3,
        scratch_shapes=[pltpu.SemaphoreType.DMA((3, 3))],
        compiler_params=pltpu.CompilerParams(vmem_limit_bytes=SMALL_LIMIT),
        cost_estimate=pl.CostEstimate(
            flops=rows * length, bytes_accessed=24 * rows * length, transcendentals=0
        ),
        name="split",
    )(starts, couplings)


def edge_masks(rows):
    lane = lax.broadcasted_iota(jnp.int32, (rows, LANES), 1)
    return lane, lane == 0, lane == LANES - 1


def over(rows, length, base, visits):
    count = length // LANES - 2 * base
    size = group_of(count)

    def step(group, totals):
        start = (base + group * size) * LANES
        totals = list(totals)

        def tile_at(tile):
            offset = start + tile * LANES
            if base == 0 and tile < 0:
                offset = jnp.maximum(offset, 0)
            if base == 0 and tile >= size:
                offset = jnp.minimum(offset, length - LANES)
            return lanes_at(offset)

        for tile in range(size):
            for index, visit in enumerate(visits):
                share = visit(tile_at, tile)
                if share is None:
                    continue
                if base == 0 and tile == 0:
                    share = jnp.where(group == 0, 0.0, share)
                if base == 0 and tile == size - 1:
                    share = jnp.where(group == count // size - 1, 0.0, share)
                totals[index] = totals[index] + share
        return tuple(totals)

    zero = jnp.zeros((rows, LANES), jnp.float32)
    return lax.fori_loop(0, count // size, step, (zero,) * len(visits))


def keep(ref):
    def store(index, at, value):
        ref[0, index, :, at] = value
        ref[1, index, :, at] = pltpu.roll(value, LANES - 1, 1)
        ref[2, index, :, at] = pltpu.roll(value, 1, 1)

    return store


def opening(coupling, left_coupling, start, refs, store, nodes):
    _, is_first, is_last = edge_masks(coupling.shape[0])
    here, ahead, behind = refs

    def visit(tile_at, tile):
        at, above, below = tile_at(tile), tile_at(tile + 1), tile_at(tile - 1)
        value = here[:, at]
        right = jnp.where(is_last, ahead[:, above], ahead[:, at])
        left = jnp.where(is_first, behind[:, below], behind[:, at])
        square = value * value
        flow = coupling[:, at] * (right - value) - left_coupling[:, at] * (value - left)
        slope = flow + (value - value * square)
        origin = start(at)
        share = None
        for index in nodes:
            base = origin + slope * ROW_SUMS[index]
            defect = base - value
            share = defect * defect if share is None else share + defect * defect
            store(index, at, newton_steps(base, value, square, IMPLICIT[index]))
        return share

    return visit


def later(coupling, left_coupling, start, ref, store, nodes):
    _, is_first, is_last = edge_masks(coupling.shape[0])

    def visit(tile_at, tile):
        at, above, below = tile_at(tile), tile_at(tile + 1), tile_at(tile - 1)
        values, squares, slopes = [], [], []
        for index in range(M):
            value = ref[0, index, :, at]
            right = jnp.where(is_last, ref[1, index, :, above], ref[1, index, :, at])
            left = jnp.where(is_first, ref[2, index, :, below], ref[2, index, :, at])
            square = value * value
            flow = coupling[:, at] * (right - value) - left_coupling[:, at] * (value - left)
            values.append(value)
            squares.append(square)
            slopes.append(flow + (value - value * square))
        origin = start(at)
        share = None
        for index in nodes:
            base = origin + weighted(slopes, WEIGHTS[index])
            defect = base - values[index]
            share = defect * defect if share is None else share + defect * defect
            store(index, at, newton_steps(base, values[index], squares[index], IMPLICIT[index]))
        return share

    return visit


def inner(at):
    return pl.ds(at.start - LANES, LANES)


def emit(done):
    def store(index, at, value):
        done[index, :, inner(at)] = value

    return store


def shifted_by(at, offset):
    return lanes_at(at.start + offset)


def early_kernel(
    chunk, near, mine, partner, straight, crossed,
    ending, w_lo, coupling, left_coupling, done, residual,
    v_lo, v_lo_ahead, v_lo_behind, v_hi, v_hi_ahead, v_hi_behind,
    v_h1, v_h1_ahead, v_h1_behind, v_h2, e_h1, u_lo, u_hi, w_hi,
):
    side, pair, _ = place()
    first = pair == 0
    even = side == 0
    rows, length = coupling.shape
    core = length - 2 * LANES
    _, is_first, _ = edge_masks(rows)

    def prepare(tile_at, tile):
        at, below = tile_at(tile), tile_at(tile - 1)
        wide = shifted_by(at, chunk * core)
        own = near[:, wide]
        coupling[:, at] = own
        left_coupling[:, at] = jnp.where(
            is_first, pltpu.roll(near[:, shifted_by(below, chunk * core)], 1, 1),
            pltpu.roll(own, 1, 1),
        )
        for pick, here, ahead, behind in (
            ((mine, partner), v_lo, v_lo_ahead, v_lo_behind),
            ((partner, mine), v_hi, v_hi_ahead, v_hi_behind),
            ((crossed, straight), v_h1, v_h1_ahead, v_h1_behind),
        ):
            value = jnp.where(even, pick[0][:, wide], pick[1][:, wide])
            here[:, at] = value
            ahead[:, at] = pltpu.roll(value, LANES - 1, 1)
            behind[:, at] = pltpu.roll(value, 1, 1)
        v_h2[:, at] = jnp.where(even, straight[:, wide], crossed[:, wide])

    over(rows, length, 0, [prepare])

    def keep_end(index, at, value):
        e_h1[:, at] = value

    pieces = (coupling, left_coupling)
    every = range(M)
    _, lo_0, hi_0 = over(
        rows,
        length,
        0,
        [
            opening(
                *pieces, lambda s: v_h2[:, s], (v_h1, v_h1_ahead, v_h1_behind), keep_end, [LAST]
            ),
            opening(
                *pieces,
                lambda s: jnp.where(first, v_lo[:, s], v_h1[:, s]),
                (v_lo, v_lo_ahead, v_lo_behind), keep(u_lo), every,
            ),
            opening(
                *pieces, lambda s: v_lo[:, s], (v_hi, v_hi_ahead, v_hi_behind), keep(u_hi), every
            ),
        ],
    )
    lo_1, hi_1 = over(
        rows,
        length,
        0,
        [
            later(
                *pieces,
                lambda s: jnp.where(first, v_lo[:, s], e_h1[:, s]),
                u_lo, keep(w_lo), every,
            ),
            later(*pieces, lambda s: u_lo[0, LAST, :, s], u_hi, keep(w_hi), every),
        ],
    )

    def last(tile_at, tile):
        at = tile_at(tile)
        ending[:, inner(at)] = w_hi[0, LAST, :, at]
        return third(tile_at, tile)

    third = later(*pieces, lambda s: w_lo[0, LAST, :, s], w_hi, emit(done), every)
    (hi_2,) = over(rows, length, 1, [last])
    residual[0] = lo_0 + hi_0
    residual[1] = lo_1 + hi_1
    residual[2] = hi_2


def late_kernel(
    chunk, mine, partner, ending, w_lo, coupling, left_coupling, done, before, *refs
):
    outs, (residual, fresh) = refs[: 2 * M], refs[2 * M :]
    side, pair, node = place()
    first = pair == 0
    even = side == 0
    rows, length = coupling.shape
    core = length - 2 * LANES

    def start(s):
        wide = shifted_by(s, chunk * core)
        begun = jnp.where(even, mine[:, wide], partner[:, wide])
        return jnp.where(first, begun, ending[:, inner(s)])

    (lo_2,) = over(
        rows,
        length,
        1,
        [later(coupling, left_coupling, start, w_lo, emit(fresh), range(M))],
    )
    residual[0] = before[0]
    residual[1] = before[1]
    residual[2] = before[2] + lo_2

    def hand_over(lo_flip):
        def copy(tile_at, tile):
            at = inner(tile_at(tile))
            for other in range(M):
                outs[lo_flip * M + other][:, at] = fresh[other ^ node, :, at]
                outs[(1 - lo_flip) * M + other][:, at] = done[other ^ node, :, at]

        over(rows, length, 1, [copy])

    for index in range(2):

        @pl.when(side == index)
        def _(index=index):
            hand_over(index)


def run_early(chunk, near, pieces, core):
    rows = near.shape[0]
    length = core + 2 * LANES
    shape = jax.ShapeDtypeStruct
    flat = pltpu.VMEM((rows, length), jnp.float32)
    deep = pltpu.VMEM((3, M, rows, length), jnp.float32)
    vmem = pl.BlockSpec(memory_space=pltpu.VMEM)
    return pl.pallas_call(
        functools.partial(early_kernel, chunk),
        out_shape=[
            shape((rows, core), jnp.float32),
            shape((3, M, rows, length), jnp.float32),
            shape((rows, length), jnp.float32),
            shape((rows, length), jnp.float32),
            shape((M, rows, core), jnp.float32),
            shape((SWEEPS, rows, LANES), jnp.float32),
        ],
        in_specs=[vmem] * (1 + len(pieces)),
        out_specs=[vmem] * 6,
        scratch_shapes=[flat] * 11 + [deep] * 3,
        compiler_params=pltpu.CompilerParams(vmem_limit_bytes=LARGE_LIMIT),
        cost_estimate=pl.CostEstimate(
            flops=800 * rows * length, bytes_accessed=64 * rows * length, transcendentals=0
        ),
        name="early",
    )(near, *pieces)


def run_late(chunk, mine, partner, ending, state):
    rows, core = ending.shape
    shape = jax.ShapeDtypeStruct
    vmem = pl.BlockSpec(memory_space=pltpu.VMEM)
    results = pl.pallas_call(
        functools.partial(late_kernel, chunk),
        out_shape=[shape((rows, core), jnp.float32)] * (2 * M)
        + [shape((SWEEPS, rows, LANES), jnp.float32)],
        in_specs=[vmem] * (3 + len(state)),
        out_specs=[vmem] * (2 * M + 1),
        scratch_shapes=[pltpu.VMEM((M, rows, core), jnp.float32)],
        compiler_params=pltpu.CompilerParams(vmem_limit_bytes=LARGE_LIMIT),
        cost_estimate=pl.CostEstimate(
            flops=200 * rows * core, bytes_accessed=64 * rows * core, transcendentals=0
        ),
        name="late",
    )(mine, partner, ending, *state)
    return results[: 2 * M], results[2 * M]


def gather_kernel(half, start, count, *refs):
    blocks = refs[:count]
    out, save = refs[-2:]
    side, _, node = place()
    rows, chunk = blocks[0].shape
    copies = []
    for index, block in enumerate(blocks):
        flip, other = index // M, index % M
        column = (side if flip == 0 else 1 - side) * half + start
        target = out.at[
            pl.ds(pl.multiple_of((other ^ node) * rows, rows), rows),
            pl.ds(pl.multiple_of(column, LANES), chunk),
        ]
        copies.append(pltpu.make_async_copy(block, target, save.at[index]))
    for copy in copies:
        copy.start()
    for copy in copies:
        copy.wait()


def gather_blocks(blocks, result, half, start, systems):
    rows, chunk = blocks[0].shape
    count = len(blocks)
    hbm = pl.BlockSpec(memory_space=pltpu.HBM)
    vmem = pl.BlockSpec(memory_space=pltpu.VMEM)
    previous = [] if result is None else [result]
    return pl.pallas_call(
        functools.partial(gather_kernel, half, start, count),
        out_shape=jax.ShapeDtypeStruct((systems, 2 * half), jnp.float32),
        in_specs=[vmem] * count + [hbm] * len(previous),
        out_specs=hbm,
        scratch_shapes=[pltpu.SemaphoreType.DMA((count,))],
        input_output_aliases={} if result is None else {count: 0},
        compiler_params=pltpu.CompilerParams(vmem_limit_bytes=SMALL_LIMIT),
        cost_estimate=pl.CostEstimate(
            flops=count * rows * chunk, bytes_accessed=8 * count * rows * chunk, transcendentals=0
        ),
        name="assemble",
    )(*blocks, *previous)


def body(slice_starts, coupling):
    slices = lax.axis_size("tm")
    systems, cells = coupling.shape
    rows = systems // M
    half = cells // 2
    chunk = half // CHUNKS
    count = slices * M

    def moved(value, target):
        pairs = [(i, target(i)) for i in range(slices)]
        return lax.ppermute(value, "tm", [(i, j) for i, j in pairs if 0 <= j < slices])

    mine, other, near = split_starts(slice_starts[0], coupling, rows, half + 2 * LANES)
    pieces = (
        mine,
        moved(other, lambda i: i ^ 1),
        moved(mine, lambda i: i + 2),
        moved(other, lambda i: (i ^ 1) + 2),
    )
    states, endings = [], []
    for index in range(CHUNKS):
        ending, *state = run_early(index, near, pieces, chunk)
        endings.append(moved(ending, lambda i: i + 2))
        states.append(state)
    partial = None
    result = None
    for index in range(CHUNKS):
        outs, sums = run_late(index, pieces[0], pieces[1], endings[index], states[index])
        partial = sums if partial is None else partial + sums
        blocks = [outs[0]]
        for step in range(1, 2 * M):
            pairs = [(i, i ^ step) for i in range(count)]
            blocks.append(lax.ppermute(outs[step], ("tm", "node"), pairs))
        result = gather_blocks(blocks, result, half, index * chunk, systems)

    sums = jnp.sum(partial, axis=2)
    flat = jnp.pad(sums.reshape(-1), (0, -sums.size % LANES))
    shared = lax.all_to_all(
        jnp.broadcast_to(flat[None], (count, flat.shape[0])), ("tm", "node"), 0, 0
    )
    summed = jnp.sum(shared.reshape(slices, M, -1), axis=0)[:, : sums.size]
    summed = summed.reshape(M, SWEEPS, rows).transpose(1, 0, 2).reshape(SWEEPS, systems)
    residual_log = jnp.log(log_floor + summed / (slices * M * cells))
    return (result[None, None], residual_log)


def solution(mesh):
    placed = (P("tm", None, None), P())

    return jax.shard_map(
        body,
        mesh=mesh,
        in_specs=placed,
        out_specs=(P("tm", "node", None, None), P()),
        check_vma=False,
    )
```

```python
import functools

import jax
import jax.numpy as jnp
from jax import lax
from jax.experimental import pallas as pl
from jax.experimental.pallas import tpu as pltpu
from jax.sharding import PartitionSpec as P


M = 4
SWEEPS = 3
NEWTON = 2
LANES = 128
GROUP = 22
HOME_ORDER = sorted(range(1, 2 * M), key=lambda step: (step % 2, -step))
LARGE_LIMIT = 24 * 1024 * 1024
SMALL_LIMIT = 8 * 1024 * 1024

time_step = 0.5
log_floor = 0.05


def legendre_gap(point, node_count):
    before = 1.0
    current = point
    for degree in range(1, node_count):
        following = ((2 * degree + 1) * point * current - degree * before) / (degree + 1)
        before = current
        current = following
    return current - before


def collocation(node_count):
    points = []
    samples = 4000
    for sample_index in range(samples - 1):
        lower_end = -1.0 + 2.0 * sample_index / samples
        upper_end = -1.0 + 2.0 * (sample_index + 1) / samples
        lower_value = legendre_gap(lower_end, node_count)
        upper_value = legendre_gap(upper_end, node_count)
        if lower_value * upper_value < 0.0:
            for _ in range(80):
                middle = 0.5 * (lower_end + upper_end)
                middle_value = legendre_gap(middle, node_count)
                if lower_value * middle_value <= 0.0:
                    upper_end = middle
                else:
                    lower_end = middle
                    lower_value = middle_value
            points.append(0.5 * (lower_end + upper_end))
    points.append(1.0)
    node_times = [(point + 1.0) / 2.0 for point in points]
    matrix = [[0.0] * node_count for _ in range(node_count)]
    for column in range(node_count):
        coeffs = [1.0]
        for other in range(node_count):
            if other != column:
                scale = node_times[column] - node_times[other]
                shifted = [0.0] + coeffs
                scaled = [value * node_times[other] for value in coeffs] + [0.0]
                coeffs = [(shifted[power] - scaled[power]) / scale for power in range(len(shifted))]
        for row_index in range(node_count):
            upper_time = node_times[row_index]
            matrix[row_index][column] = sum(
                (
                    coeffs[power] * upper_time ** (power + 1) / (power + 1)
                    for power in range(len(coeffs))
                )
            )
    return (node_times, matrix)


NODE_TIMES, MATRIX = collocation(M)
LAST = M - 1
WEIGHTS = [[time_step * entry for entry in row] for row in MATRIX]
ROW_SUMS = [time_step * moment for moment in NODE_TIMES]
IMPLICIT = [time_step * moment / M for moment in NODE_TIMES]


def newton_steps(base, value, square, weight):
    rest = base - weight * value
    tripled = square * (3.0 * weight)
    cubic = tripled * value
    target = rest + cubic * (1.0 / 3.0)
    value = (rest + cubic) / (tripled + (1.0 - weight))
    for _ in range(1, NEWTON):
        tripled = (value * value) * (3.0 * weight)
        numerator = target + (tripled * value) * (2.0 / 3.0)
        value = numerator / (tripled + (1.0 - weight))
    return value


def weighted(terms, row):
    total = terms[0] * row[0]
    for term, entry in zip(terms[1:], row[1:]):
        total = total + term * entry
    return total


def group_of(count):
    return max(size for size in range(1, GROUP + 1) if count % size == 0)


def lanes_at(offset):
    return pl.ds(pl.multiple_of(offset, LANES), LANES)


def tracks(source, target, row, column, cells, core, sem):
    rows = target.shape[0]
    part = source.at[pl.ds(pl.multiple_of(row, rows), rows), :]
    before = pl.multiple_of(lax.rem(column + (cells - LANES), cells), LANES)
    after = pl.multiple_of(lax.rem(column + core, cells), LANES)
    middle = pl.multiple_of(column, LANES)
    return [
        pltpu.make_async_copy(
            part.at[:, pl.ds(before, LANES)], target.at[:, pl.ds(0, LANES)], sem.at[0]
        ),
        pltpu.make_async_copy(
            part.at[:, pl.ds(middle, core)], target.at[:, pl.ds(LANES, core)], sem.at[1]
        ),
        pltpu.make_async_copy(
            part.at[:, pl.ds(after, LANES)],
            target.at[:, pl.ds(LANES + core, LANES)],
            sem.at[2],
        ),
    ]


def place():
    position = lax.axis_index("tm")
    return lax.rem(position, 2), lax.div(position, 2), lax.axis_index("node")


def split_kernel(starts, couplings, mine, other, near, sems):
    side, _, node = place()
    rows, length = mine.shape
    cells = starts.shape[1]
    core = length - 2 * LANES
    copies = []
    for slot, (source, target, which) in enumerate(
        ((starts, mine, side), (starts, other, 1 - side), (couplings, near, side))
    ):
        copies += tracks(source, target, node * rows, which * core, cells, core, sems.at[slot])
    for copy in copies:
        copy.start()
    for copy in copies:
        copy.wait()


def split_starts(starts, couplings, rows, length):
    return pl.pallas_call(
        split_kernel,
        out_shape=[jax.ShapeDtypeStruct((rows, length), jnp.float32)] * 3,
        in_specs=[pl.BlockSpec(memory_space=pltpu.HBM)] * 2,
        out_specs=[pl.BlockSpec(memory_space=pltpu.VMEM)] * 3,
        scratch_shapes=[pltpu.SemaphoreType.DMA((3, 3))],
        compiler_params=pltpu.CompilerParams(vmem_limit_bytes=SMALL_LIMIT),
        cost_estimate=pl.CostEstimate(
            flops=rows * length, bytes_accessed=24 * rows * length, transcendentals=0
        ),
        name="split",
    )(*(pltpu.with_memory_space_constraint(a, pltpu.HBM) for a in (starts, couplings)))


def edge_masks(rows):
    lane = lax.broadcasted_iota(jnp.int32, (rows, LANES), 1)
    return lane, lane == 0, lane == LANES - 1


def over(rows, length, base, visits):
    count = length // LANES - 2 * base
    size = group_of(count)

    def step(group, totals):
        start = (base + group * size) * LANES
        totals = list(totals)

        def tile_at(tile):
            offset = start + tile * LANES
            if base == 0 and tile < 0:
                offset = jnp.maximum(offset, 0)
            if base == 0 and tile >= size:
                offset = jnp.minimum(offset, length - LANES)
            return lanes_at(offset)

        for tile in range(size):
            for index, visit in enumerate(visits):
                share = visit(tile_at, tile)
                if share is None:
                    continue
                if base == 0 and tile == 0:
                    share = jnp.where(group == 0, 0.0, share)
                if base == 0 and tile == size - 1:
                    share = jnp.where(group == count // size - 1, 0.0, share)
                totals[index] = totals[index] + share
        return tuple(totals)

    zero = jnp.zeros((rows, LANES), jnp.float32)
    return lax.fori_loop(0, count // size, step, (zero,) * len(visits))


def keep(ref):
    def store(index, at, value):
        ref[0, index, :, at] = value
        ref[1, index, :, at] = pltpu.roll(value, LANES - 1, 1)
        ref[2, index, :, at] = pltpu.roll(value, 1, 1)

    return store


def neighbours(masks, ahead, behind, at, above, below):
    is_first, is_last = masks
    return (
        jnp.where(is_last, ahead[:, above], ahead[:, at]),
        jnp.where(is_first, behind[:, below], behind[:, at]),
    )


def opening(pieces, masks, start, refs, store, nodes):
    coupling, left_coupling, local = pieces
    here, ahead, behind = refs

    def visit(tile_at, tile):
        at, above, below = tile_at(tile), tile_at(tile + 1), tile_at(tile - 1)
        value = here[:, at]
        right, left = neighbours(masks, ahead, behind, at, above, below)
        square = value * value
        flow = coupling[:, at] * right + left_coupling[:, at] * left
        slope = flow + value * (local[:, at] - square)
        origin = start(at)
        share = None
        for index in nodes:
            base = origin + slope * ROW_SUMS[index]
            defect = base - value
            share = defect * defect if share is None else share + defect * defect
            store(index, at, newton_steps(base, value, square, IMPLICIT[index]))
        return share

    return visit


def later(pieces, masks, start, ref, store, nodes):
    coupling, left_coupling, local = pieces

    def visit(tile_at, tile):
        at, above, below = tile_at(tile), tile_at(tile + 1), tile_at(tile - 1)
        values, squares, slopes = [], [], []
        for index in range(M):
            value = ref[0, index, :, at]
            right, left = neighbours(
                masks, ref.at[1, index], ref.at[2, index], at, above, below
            )
            square = value * value
            flow = coupling[:, at] * right + left_coupling[:, at] * left
            values.append(value)
            squares.append(square)
            slopes.append(flow + value * (local[:, at] - square))
        origin = start(at)
        share = None
        for index in nodes:
            base = origin + weighted(slopes, WEIGHTS[index])
            defect = base - values[index]
            share = defect * defect if share is None else share + defect * defect
            store(index, at, newton_steps(base, values[index], squares[index], IMPLICIT[index]))
        return share

    return visit


def inner(at):
    return pl.ds(at.start - LANES, LANES)


def emit(done):
    def store(index, at, value):
        done[index, :, inner(at)] = value

    return store


def pair_kernel(
    near, mine, partner, left_coupling, local, v_lo, v_lo_ahead, v_lo_behind, u_hi, squares,
    v_hi, v_hi_ahead, v_hi_behind,
):
    side, _, _ = place()
    even = side == 0
    rows, length = near.shape
    _, is_first, is_last = edge_masks(rows)

    def prepare(tile_at, tile):
        at, below = tile_at(tile), tile_at(tile - 1)
        own = near[:, at]
        before = jnp.where(is_first, pltpu.roll(near[:, below], 1, 1), pltpu.roll(own, 1, 1))
        left_coupling[:, at] = before
        local[:, at] = 1.0 - own - before
        for picks, here, ahead, behind in (
            ((mine, partner), v_lo, v_lo_ahead, v_lo_behind),
            ((partner, mine), v_hi, v_hi_ahead, v_hi_behind),
        ):
            value = jnp.where(even, picks[0][:, at], picks[1][:, at])
            here[:, at] = value
            ahead[:, at] = pltpu.roll(value, LANES - 1, 1)
            behind[:, at] = pltpu.roll(value, 1, 1)

    over(rows, length, 0, [prepare])
    (hi_0,) = over(
        rows,
        length,
        0,
        [
            opening(
                (near, left_coupling, local), (is_first, is_last), lambda s: v_lo[:, s],
                (v_hi, v_hi_ahead, v_hi_behind), keep(u_hi), range(M),
            )
        ],
    )
    squares[...] = hi_0


def start_kernel(
    near, straight, crossed, left_coupling, local, v_lo, v_lo_ahead, v_lo_behind, u_hi, before,
    ending, e_h1, u_lo, w_hi, squares, v_h1, v_h1_ahead, v_h1_behind,
):
    side, pair, _ = place()
    first = pair == 0
    even = side == 0
    rows, length = near.shape
    _, is_first, is_last = edge_masks(rows)
    pieces, masks = (near, left_coupling, local), (is_first, is_last)

    def prepare(tile_at, tile):
        at = tile_at(tile)
        value = jnp.where(even, crossed[:, at], straight[:, at])
        v_h1[:, at] = value
        v_h1_ahead[:, at] = pltpu.roll(value, LANES - 1, 1)
        v_h1_behind[:, at] = pltpu.roll(value, 1, 1)

    over(rows, length, 0, [prepare])

    def keep_end(index, at, value):
        e_h1[:, at] = value

    _, lo_0 = over(
        rows,
        length,
        0,
        [
            opening(
                pieces, masks,
                lambda s: jnp.where(even, straight[:, s], crossed[:, s]),
                (v_h1, v_h1_ahead, v_h1_behind), keep_end, [LAST],
            ),
            opening(
                pieces, masks,
                lambda s: jnp.where(first, v_lo[:, s], v_h1[:, s]),
                (v_lo, v_lo_ahead, v_lo_behind), keep(u_lo), range(M),
            ),
        ],
    )
    (hi_1,) = over(
        rows,
        length,
        0,
        [later(pieces, masks, lambda s: u_lo[0, LAST, :, s], u_hi, keep(w_hi), range(M))],
    )

    def finish(tile_at, tile):
        at = tile_at(tile)
        ending[:, inner(at)] = w_hi[0, LAST, :, at]

    over(rows, length, 1, [finish])
    squares[0] = before[...] + lo_0
    squares[1] = hi_1


def middle_kernel(
    near, left_coupling, local, v_lo, e_h1, u_lo, w_hi, before, w_lo, done, squares
):
    _, pair, _ = place()
    first = pair == 0
    rows, length = near.shape
    _, is_first, is_last = edge_masks(rows)
    pieces, masks = (near, left_coupling, local), (is_first, is_last)
    (lo_1,) = over(
        rows,
        length,
        0,
        [
            later(
                pieces, masks,
                lambda s: jnp.where(first, v_lo[:, s], e_h1[:, s]),
                u_lo, keep(w_lo), range(M),
            )
        ],
    )
    (hi_2,) = over(
        rows,
        length,
        1,
        [later(pieces, masks, lambda s: w_lo[0, LAST, :, s], w_hi, emit(done), range(M))],
    )
    squares[0] = before[0]
    squares[1] = before[1] + lo_1
    squares[2] = hi_2


def late_kernel(near, left_coupling, local, v_lo, ending, w_lo, done, before, *refs):
    outs, (payload, fresh) = refs[: 2 * M], refs[2 * M :]
    side, pair, node = place()
    first = pair == 0
    rows, length = near.shape
    lane, is_first, is_last = edge_masks(rows)
    (lo_2,) = over(
        rows,
        length,
        1,
        [
            later(
                (near, left_coupling, local), (is_first, is_last),
                lambda s: jnp.where(first, v_lo[:, s], ending[:, inner(s)]),
                w_lo, emit(fresh), range(M),
            )
        ],
    )

    def hand_over(lo_flip):
        def copy(tile_at, tile):
            at = inner(tile_at(tile))
            for other in range(M):
                outs[lo_flip * M + other][:, at] = fresh[other ^ node, :, at]
                outs[(1 - lo_flip) * M + other][:, at] = done[other ^ node, :, at]

        over(rows, length, 1, [copy])

    for index in range(2):

        @pl.when(side == index)
        def _(index=index):
            hand_over(index)

    system = lax.broadcasted_iota(jnp.int32, (rows, LANES), 0)
    mine = lane == node * rows + system
    shares = []
    for index in range(SWEEPS):
        total = before[index] + lo_2 if index == SWEEPS - 1 else before[index]
        column = jnp.where(mine, jnp.sum(total, axis=1, keepdims=True), 0.0)
        shares.append(jnp.sum(column, axis=0, keepdims=True))
    tile = jnp.concatenate(
        shares + [jnp.zeros((payload.shape[1] - SWEEPS, LANES), jnp.float32)], axis=0
    )
    for index in range(payload.shape[0]):
        payload[index] = tile


def call(kernel, operands, results, scratch, flops, limit):
    vmem = pl.BlockSpec(memory_space=pltpu.VMEM)
    return pl.pallas_call(
        kernel,
        out_shape=[jax.ShapeDtypeStruct(shape, jnp.float32) for shape in results],
        in_specs=[vmem] * len(operands),
        out_specs=[vmem] * len(results),
        scratch_shapes=[pltpu.VMEM(shape, jnp.float32) for shape in scratch],
        compiler_params=pltpu.CompilerParams(vmem_limit_bytes=limit),
        cost_estimate=pl.CostEstimate(flops=flops, bytes_accessed=flops, transcendentals=0),
    )(*operands)


def final_kernel(scale, count, shared, *refs):
    blocks = refs[:count]
    out, residual, save = refs[count:]
    side, _, node = place()
    rows, half = blocks[0].shape
    copies = []
    for index, block in enumerate(blocks):
        flip, other = index // M, index % M
        column = (side if flip == 0 else 1 - side) * half
        target = out.at[
            pl.ds(pl.multiple_of((other ^ node) * rows, rows), rows),
            pl.ds(pl.multiple_of(column, LANES), half),
        ]
        copies.append(pltpu.make_async_copy(block, target, save.at[index]))
    for copy in copies:
        copy.start()
    total = shared[0]
    for index in range(1, shared.shape[0]):
        total = total + shared[index]
    logs = jnp.log(log_floor + total / scale)
    residual[...] = logs[: residual.shape[0], : residual.shape[1]]
    for copy in copies:
        copy.wait()


def finish(shared, blocks, systems, scale):
    rows, half = blocks[0].shape
    count = len(blocks)
    vmem = pl.BlockSpec(memory_space=pltpu.VMEM)
    return pl.pallas_call(
        functools.partial(final_kernel, scale, count),
        out_shape=[
            jax.ShapeDtypeStruct((systems, 2 * half), jnp.float32),
            jax.ShapeDtypeStruct((SWEEPS, systems), jnp.float32),
        ],
        in_specs=[vmem] * (1 + count),
        out_specs=[pl.BlockSpec(memory_space=pltpu.HBM), vmem],
        scratch_shapes=[pltpu.SemaphoreType.DMA((count,))],
        compiler_params=pltpu.CompilerParams(vmem_limit_bytes=SMALL_LIMIT),
        cost_estimate=pl.CostEstimate(
            flops=count * rows * half, bytes_accessed=8 * count * rows * half, transcendentals=0
        ),
        name="finish",
    )(shared, *blocks)


def body(slice_starts, coupling):
    slices = lax.axis_size("tm")
    systems, cells = coupling.shape
    rows = systems // M
    half = cells // 2
    length = half + 2 * LANES
    count = slices * M
    flat, wide, core = (rows, length), (3, M, rows, length), (rows, half)
    small = (rows, LANES)

    def moved(value, target):
        pairs = [(i, target(i)) for i in range(slices)]
        return lax.ppermute(value, "tm", [(i, j) for i, j in pairs if 0 <= j < slices])

    mine, other, near = split_starts(slice_starts[0], coupling, rows, length)
    partner = moved(other, lambda i: i ^ 1)
    crossed = moved(other, lambda i: (i ^ 1) + 2)
    straight = moved(mine, lambda i: i + 2)
    left_coupling, local, *v_lo, u_hi, squares = call(
        pair_kernel, (near, mine, partner),
        [flat] * 5 + [wide, small], [flat] * 3, 200 * rows * length, LARGE_LIMIT,
    )
    ending, e_h1, u_lo, w_hi, squares = call(
        start_kernel,
        (near, straight, crossed, left_coupling, local, *v_lo, u_hi, squares),
        [core, flat, wide, wide, (2,) + small], [flat] * 3, 400 * rows * length, LARGE_LIMIT,
    )
    ending = moved(ending, lambda i: i + 2)
    w_lo, done, squares = call(
        middle_kernel,
        (near, left_coupling, local, v_lo[0], e_h1, u_lo, w_hi, squares),
        [wide, (M,) + core, (SWEEPS,) + small], [], 400 * rows * length, LARGE_LIMIT,
    )
    *outs, payload = call(
        late_kernel,
        (near, left_coupling, local, v_lo[0], ending, w_lo, done, squares),
        [core] * (2 * M) + [(count, 8, LANES)], [(M,) + core], 200 * rows * length,
        LARGE_LIMIT,
    )
    blocks = list(outs)
    for step in HOME_ORDER:
        pairs = [(i, i ^ step) for i in range(count)]
        blocks[step] = lax.ppermute(outs[step], ("tm", "node"), pairs)
    shared = lax.all_to_all(payload, ("tm", "node"), 0, 0)
    result, residual_log = finish(shared, blocks, systems, slices * M * cells)
    return (result[None, None], residual_log)


def solution(mesh):
    placed = (P("tm", None, None), P())

    return jax.shard_map(
        body,
        mesh=mesh,
        in_specs=placed,
        out_specs=(P("tm", "node", None, None), P()),
        check_vma=False,
    )
```

```python
import functools

import jax
import jax.numpy as jnp
from jax import lax
from jax.experimental import pallas as pl
from jax.experimental.pallas import tpu as pltpu
from jax.sharding import PartitionSpec as P


M = 4
SWEEPS = 3
NEWTON = 2
LANES = 128
GROUP = 66
LARGE_LIMIT = 24 * 1024 * 1024
SMALL_LIMIT = 8 * 1024 * 1024

time_step = 0.5
log_floor = 0.05


def legendre_gap(point, node_count):
    before = 1.0
    current = point
    for degree in range(1, node_count):
        following = ((2 * degree + 1) * point * current - degree * before) / (degree + 1)
        before = current
        current = following
    return current - before


def collocation(node_count):
    points = []
    samples = 4000
    for sample_index in range(samples - 1):
        lower_end = -1.0 + 2.0 * sample_index / samples
        upper_end = -1.0 + 2.0 * (sample_index + 1) / samples
        lower_value = legendre_gap(lower_end, node_count)
        upper_value = legendre_gap(upper_end, node_count)
        if lower_value * upper_value < 0.0:
            for _ in range(80):
                middle = 0.5 * (lower_end + upper_end)
                middle_value = legendre_gap(middle, node_count)
                if lower_value * middle_value <= 0.0:
                    upper_end = middle
                else:
                    lower_end = middle
                    lower_value = middle_value
            points.append(0.5 * (lower_end + upper_end))
    points.append(1.0)
    node_times = [(point + 1.0) / 2.0 for point in points]
    matrix = [[0.0] * node_count for _ in range(node_count)]
    for column in range(node_count):
        coeffs = [1.0]
        for other in range(node_count):
            if other != column:
                scale = node_times[column] - node_times[other]
                shifted = [0.0] + coeffs
                scaled = [value * node_times[other] for value in coeffs] + [0.0]
                coeffs = [(shifted[power] - scaled[power]) / scale for power in range(len(shifted))]
        for row_index in range(node_count):
            upper_time = node_times[row_index]
            matrix[row_index][column] = sum(
                (
                    coeffs[power] * upper_time ** (power + 1) / (power + 1)
                    for power in range(len(coeffs))
                )
            )
    return (node_times, matrix)


NODE_TIMES, MATRIX = collocation(M)
LAST = M - 1
WEIGHTS = [[time_step * entry for entry in row] for row in MATRIX]
ROW_SUMS = [time_step * moment for moment in NODE_TIMES]
IMPLICIT = [time_step * moment / M for moment in NODE_TIMES]


def newton_steps(base, value, square, weight):
    rest = base - weight * value
    tripled = square * (3.0 * weight)
    cubic = tripled * value
    target = rest + cubic * (1.0 / 3.0)
    value = (rest + cubic) / (tripled + (1.0 - weight))
    for _ in range(1, NEWTON):
        tripled = (value * value) * (3.0 * weight)
        numerator = target + (tripled * value) * (2.0 / 3.0)
        value = numerator / (tripled + (1.0 - weight))
    return value


def weighted(terms, row):
    total = terms[0] * row[0]
    for term, entry in zip(terms[1:], row[1:]):
        total = total + term * entry
    return total


def group_of(count):
    return max(size for size in range(1, GROUP + 1) if count % size == 0)


def lanes_at(offset):
    return pl.ds(pl.multiple_of(offset, LANES), LANES)


def tracks(source, target, row, column, cells, core, sem):
    rows = target.shape[0]
    part = source.at[pl.ds(pl.multiple_of(row, rows), rows), :]
    before = pl.multiple_of(lax.rem(column + (cells - LANES), cells), LANES)
    after = pl.multiple_of(lax.rem(column + core, cells), LANES)
    middle = pl.multiple_of(column, LANES)
    return [
        pltpu.make_async_copy(
            part.at[:, pl.ds(before, LANES)], target.at[:, pl.ds(0, LANES)], sem.at[0]
        ),
        pltpu.make_async_copy(
            part.at[:, pl.ds(middle, core)], target.at[:, pl.ds(LANES, core)], sem.at[1]
        ),
        pltpu.make_async_copy(
            part.at[:, pl.ds(after, LANES)],
            target.at[:, pl.ds(LANES + core, LANES)],
            sem.at[2],
        ),
    ]


def place():
    position = lax.axis_index("tm")
    return lax.rem(position, 2), lax.div(position, 2), lax.axis_index("node")


def split_kernel(source, *refs):
    targets, sems = refs[:-1], refs[-1]
    side, _, node = place()
    rows, length = targets[0].shape
    cells = source.shape[1]
    core = length - 2 * LANES
    copies = []
    for slot, target in enumerate(targets):
        which = 1 - side if slot else side
        copies += tracks(source, target, node * rows, which * core, cells, core, sems.at[slot])
    for copy in copies:
        copy.start()
    for copy in copies:
        copy.wait()


def split(source, rows, length, count):
    return pl.pallas_call(
        split_kernel,
        out_shape=[jax.ShapeDtypeStruct((rows, length), jnp.float32)] * count,
        in_specs=[pl.BlockSpec(memory_space=pltpu.HBM)],
        out_specs=[pl.BlockSpec(memory_space=pltpu.VMEM)] * count,
        scratch_shapes=[pltpu.SemaphoreType.DMA((count, 3))],
        compiler_params=pltpu.CompilerParams(vmem_limit_bytes=SMALL_LIMIT),
        cost_estimate=pl.CostEstimate(
            flops=rows * length, bytes_accessed=8 * count * rows * length, transcendentals=0
        ),
        name="split",
    )(pltpu.with_memory_space_constraint(source, pltpu.HBM))


def edge_masks(rows):
    lane = lax.broadcasted_iota(jnp.int32, (rows, LANES), 1)
    return lane, lane == 0, lane == LANES - 1


def over(rows, length, base, visits):
    count = length // LANES - 2 * base
    size = group_of(count)

    def step(group, totals):
        start = (base + group * size) * LANES
        totals = list(totals)

        def tile_at(tile):
            offset = start + tile * LANES
            if base == 0 and tile < 0:
                offset = jnp.maximum(offset, 0)
            if base == 0 and tile >= size:
                offset = jnp.minimum(offset, length - LANES)
            return lanes_at(offset)

        for tile in range(size):
            for index, visit in enumerate(visits):
                share = visit(tile_at, tile)
                if share is None:
                    continue
                if base == 0 and tile == 0:
                    share = jnp.where(group == 0, 0.0, share)
                if base == 0 and tile == size - 1:
                    share = jnp.where(group == count // size - 1, 0.0, share)
                totals[index] = totals[index] + share
        return tuple(totals)

    zero = jnp.zeros((rows, LANES), jnp.float32)
    return lax.fori_loop(0, count // size, step, (zero,) * len(visits))


def keep(ref):
    def store(index, at, value):
        ref[0, index, :, at] = value
        ref[1, index, :, at] = pltpu.roll(value, LANES - 1, 1)
        ref[2, index, :, at] = pltpu.roll(value, 1, 1)

    return store


def neighbours(masks, ahead, behind, at, above, below):
    is_first, is_last = masks
    return (
        jnp.where(is_last, ahead[:, above], ahead[:, at]),
        jnp.where(is_first, behind[:, below], behind[:, at]),
    )


def slope_at(pieces, masks, here, ahead, behind, tile_at, tile):
    coupling, left_coupling, local = pieces
    at, above, below = tile_at(tile), tile_at(tile + 1), tile_at(tile - 1)
    value = here[:, at]
    right, left = neighbours(masks, ahead, behind, at, above, below)
    square = value * value
    flow = coupling[:, at] * right + left_coupling[:, at] * left
    return value, square, flow + value * (local[:, at] - square)


def squared(total, defect):
    return defect * defect if total is None else total + defect * defect


def opening(pieces, masks, start, refs, store, nodes):
    def visit(tile_at, tile):
        at = tile_at(tile)
        value, square, slope = slope_at(pieces, masks, *refs, tile_at, tile)
        origin = start(at)
        share = None
        for index in nodes:
            base = origin + slope * ROW_SUMS[index]
            share = squared(share, base - value)
            store(index, at, newton_steps(base, value, square, IMPLICIT[index]))
        return share

    return visit


def slopes_of(pieces, masks, ref, tile_at, tile):
    return [
        slope_at(
            pieces, masks, ref.at[0, index], ref.at[1, index], ref.at[2, index], tile_at, tile
        )
        for index in range(M)
    ]


def terms(pieces, masks, ref, store):
    def visit(tile_at, tile):
        at = tile_at(tile)
        slopes = [entry[2] for entry in slopes_of(pieces, masks, ref, tile_at, tile)]
        for index in range(M):
            store(index, at, weighted(slopes, WEIGHTS[index]))

    return visit


def later(pieces, masks, start, ref, store):
    def visit(tile_at, tile):
        at = tile_at(tile)
        fields = slopes_of(pieces, masks, ref, tile_at, tile)
        slopes = [entry[2] for entry in fields]
        origin = start(at)
        share = None
        for index in range(M):
            value, square, _ = fields[index]
            base = origin + weighted(slopes, WEIGHTS[index])
            share = squared(share, base - value)
            store(index, at, newton_steps(base, value, square, IMPLICIT[index]))
        return share

    return visit


def inner(at):
    return pl.ds(at.start - LANES, LANES)


def whole(ref):
    def store(index, at, value):
        ref[index, :, at] = value

    return store


def emit(done):
    def store(index, at, value):
        done[index, :, inner(at)] = value

    return store


def pair_kernel(
    near, mine, partner,
    left_coupling, local, v_lo, slope_lo, u_hi, terms_hi, squares,
    v_lo_ahead, v_lo_behind, v_hi, v_hi_ahead, v_hi_behind,
):
    side, _, _ = place()
    even = side == 0
    rows, length = near.shape
    _, is_first, is_last = edge_masks(rows)
    pieces, masks = (near, left_coupling, local), (is_first, is_last)

    def prepare(tile_at, tile):
        at, below = tile_at(tile), tile_at(tile - 1)
        own = near[:, at]
        before = jnp.where(is_first, pltpu.roll(near[:, below], 1, 1), pltpu.roll(own, 1, 1))
        left_coupling[:, at] = before
        local[:, at] = 1.0 - own - before
        for picks, here, ahead, behind in (
            ((mine, partner), v_lo, v_lo_ahead, v_lo_behind),
            ((partner, mine), v_hi, v_hi_ahead, v_hi_behind),
        ):
            value = jnp.where(even, picks[0][:, at], picks[1][:, at])
            here[:, at] = value
            ahead[:, at] = pltpu.roll(value, LANES - 1, 1)
            behind[:, at] = pltpu.roll(value, 1, 1)

    over(rows, length, 0, [prepare])

    def slopes(tile_at, tile):
        at = tile_at(tile)
        slope_lo[:, at] = slope_at(
            pieces, masks, v_lo, v_lo_ahead, v_lo_behind, tile_at, tile
        )[2]

    hi_0, _ = over(
        rows,
        length,
        0,
        [
            opening(
                pieces, masks, lambda s: v_lo[:, s],
                (v_hi, v_hi_ahead, v_hi_behind), keep(u_hi), range(M),
            ),
            slopes,
        ],
    )
    over(rows, length, 0, [terms(pieces, masks, u_hi, whole(terms_hi))])
    squares[...] = hi_0


def first_step(index, origin, slope, value):
    base = origin + slope * ROW_SUMS[index]
    return base, newton_steps(base, value, value * value, IMPLICIT[index])


def later_step(index, origin, state, integrals, at, where):
    value = state[0, index, :, at]
    base = origin + integrals[index, :, where]
    return base - value, newton_steps(base, value, value * value, IMPLICIT[index])


def start_kernel(straight, crossed, v_lo, slope_lo, u_hi, terms_hi, ending):
    side, pair, _ = place()
    first = pair == 0
    even = side == 0
    rows, length = v_lo.shape

    def visit(tile_at, tile):
        at = tile_at(tile)
        value = v_lo[:, at]
        origin = jnp.where(even, crossed[:, at], straight[:, at])
        origin = jnp.where(first, value, origin)
        _, end = first_step(LAST, origin, slope_lo[:, at], value)
        ending[:, inner(at)] = later_step(LAST, end, u_hi, terms_hi, at, at)[1]

    over(rows, length, 1, [visit])


def middle_kernel(
    near, left_coupling, local, straight, crossed, v_lo, slope_lo, u_hi, terms_hi, before,
    w_lo, w_hi, terms_lo, last_hi, squares,
    v_h1, v_h1_ahead, v_h1_behind, e_h1, u_lo,
):
    side, pair, _ = place()
    first = pair == 0
    even = side == 0
    rows, length = near.shape
    _, is_first, is_last = edge_masks(rows)
    pieces, masks = (near, left_coupling, local), (is_first, is_last)

    def prepare(tile_at, tile):
        at = tile_at(tile)
        value = jnp.where(even, crossed[:, at], straight[:, at])
        v_h1[:, at] = value
        v_h1_ahead[:, at] = pltpu.roll(value, LANES - 1, 1)
        v_h1_behind[:, at] = pltpu.roll(value, 1, 1)

    over(rows, length, 0, [prepare])

    def keep_end(index, at, value):
        e_h1[:, at] = value

    def sweep_lo(tile_at, tile):
        at = tile_at(tile)
        value, slope = v_lo[:, at], slope_lo[:, at]
        origin = jnp.where(first, value, v_h1[:, at])
        share = None
        for index in range(M):
            base, fresh = first_step(index, origin, slope, value)
            share = squared(share, base - value)
            keep(u_lo)(index, at, fresh)
        return share

    def sweep_hi(tile_at, tile):
        at = tile_at(tile)
        origin = u_lo[0, LAST, :, at]
        share = None
        for index in range(M):
            defect, fresh = later_step(index, origin, u_hi, terms_hi, at, at)
            share = squared(share, defect)
            keep(w_hi)(index, at, fresh)
        return share

    _, lo_0 = over(
        rows,
        length,
        0,
        [
            opening(
                pieces, masks,
                lambda s: jnp.where(even, straight[:, s], crossed[:, s]),
                (v_h1, v_h1_ahead, v_h1_behind), keep_end, [LAST],
            ),
            sweep_lo,
        ],
    )
    hi_1, lo_1 = over(
        rows,
        length,
        0,
        [
            sweep_hi,
            later(
                pieces, masks,
                lambda s: jnp.where(first, v_lo[:, s], e_h1[:, s]),
                u_lo, keep(w_lo),
            ),
        ],
    )
    over(
        rows,
        length,
        1,
        [
            terms(pieces, masks, w_hi, emit(last_hi)),
            terms(pieces, masks, w_lo, emit(terms_lo)),
        ],
    )
    squares[0] = before[...] + lo_0
    squares[1] = hi_1 + lo_1


def blocks_of(outs, odd, origins, states, integrals, core):
    side, _, node = place()
    half = M // 2
    nodes = [(2 * index + odd) ^ node for index in range(half)]
    weights = []
    for chosen in nodes:
        weight = jnp.float32(IMPLICIT[0])
        for index in range(1, M):
            weight = jnp.where(chosen == index, jnp.float32(IMPLICIT[index]), weight)
        weights.append(weight)

    def move(lo_flip):
        def visit(tile_at, tile):
            at = tile_at(tile)
            to = inner(at)
            for which in range(2):
                origin = origins[which](at)
                flip = lo_flip if which == 0 else 1 - lo_flip
                for index in range(half):
                    value = states[which][0, nodes[index], :, at]
                    base = origin + integrals[which][nodes[index], :, to]
                    outs[flip * half + index][:, to] = newton_steps(
                        base, value, value * value, weights[index]
                    )

        over(outs[0].shape[0], core + 2 * LANES, 1, [visit])

    for index in range(2):

        @pl.when(side == index)
        def _(index=index):
            move(index)


def origins_of(v_lo, ending, w_lo, first):
    return (
        lambda at: jnp.where(first, v_lo[:, at], ending[:, inner(at)]),
        lambda at: w_lo[0, LAST, :, at],
    )


def late_kernel(odd, v_lo, ending, w_lo, w_hi, terms_lo, last_hi, *outs):
    _, pair, _ = place()
    core = ending.shape[1]
    origins = origins_of(v_lo, ending, w_lo, pair == 0)
    blocks_of(outs, odd, origins, (w_lo, w_hi), (terms_lo, last_hi), core)


def sums_kernel(v_lo, ending, w_lo, w_hi, terms_lo, last_hi, before, payload):
    _, pair, node = place()
    rows, core = ending.shape
    lane, _, _ = edge_masks(rows)
    origins = origins_of(v_lo, ending, w_lo, pair == 0)
    states, integrals = (w_lo, w_hi), (terms_lo, last_hi)

    def defects(tile_at, tile):
        at = tile_at(tile)
        share = None
        for which in range(2):
            origin = origins[which](at)
            for index in range(M):
                base = origin + integrals[which][index, :, inner(at)]
                share = squared(share, base - states[which][0, index, :, at])
        return share

    (third,) = over(rows, core + 2 * LANES, 1, [defects])

    system = lax.broadcasted_iota(jnp.int32, (rows, LANES), 0)
    mine = lane == node * rows + system
    shares = []
    for total in (before[0], before[1], third):
        column = jnp.where(mine, jnp.sum(total, axis=1, keepdims=True), 0.0)
        shares.append(jnp.sum(column, axis=0, keepdims=True))
    payload[...] = jnp.concatenate(
        shares + [jnp.zeros((payload.shape[0] - SWEEPS, LANES), jnp.float32)], axis=0
    )


def stamp_kernel(payload, *refs):
    outs = refs[len(refs) // 2 :]
    for out in outs:
        out[:, pl.ds(out.shape[1] - LANES, LANES)] = payload[...]


def stamp(payload, blocks):
    vmem = pl.BlockSpec(memory_space=pltpu.VMEM)
    count = len(blocks)
    return pl.pallas_call(
        stamp_kernel,
        out_shape=[jax.ShapeDtypeStruct(block.shape, jnp.float32) for block in blocks],
        in_specs=[vmem] * (1 + count),
        out_specs=[vmem] * count,
        input_output_aliases={1 + index: index for index in range(count)},
        compiler_params=pltpu.CompilerParams(vmem_limit_bytes=SMALL_LIMIT),
        cost_estimate=pl.CostEstimate(flops=1024, bytes_accessed=1024, transcendentals=0),
        name="stamp",
    )(payload, *blocks)


def call(kernel, operands, results, scratch, flops, limit):
    vmem = pl.BlockSpec(memory_space=pltpu.VMEM)
    return pl.pallas_call(
        kernel,
        out_shape=[jax.ShapeDtypeStruct(shape, jnp.float32) for shape in results],
        in_specs=[vmem] * len(operands),
        out_specs=[vmem] * len(results),
        scratch_shapes=[pltpu.VMEM(shape, jnp.float32) for shape in scratch],
        compiler_params=pltpu.CompilerParams(vmem_limit_bytes=limit),
        cost_estimate=pl.CostEstimate(flops=flops, bytes_accessed=flops, transcendentals=0),
    )(*operands)


def final_kernel(half, steps, scale, *refs):
    count = len(steps)
    blocks, refs = refs[:count], refs[count:]
    if scale is None:
        out, save = refs[-2:]
    else:
        out, residual, table, save = refs[-4:]
    side, _, node = place()
    rows = blocks[0].shape[0]
    copies = []
    for index, step in enumerate(steps):
        flip, other = step // M, step % M
        column = (side if flip == 0 else 1 - side) * half
        target = out.at[
            pl.ds(pl.multiple_of((other ^ node) * rows, rows), rows),
            pl.ds(pl.multiple_of(column, LANES), half),
        ]
        copies.append(
            pltpu.make_async_copy(blocks[index].at[:, pl.ds(0, half)], target, save.at[index])
        )
    for copy in copies:
        copy.start()
    if scale is not None:
        sums = [block[:, pl.ds(half, LANES)] for block in blocks + refs[: M - count]]
        total = sums[0]
        for entry in sums[1:]:
            total = total + entry
        logs = jnp.log(log_floor + total / scale)
        table[...] = logs[: table.shape[0], : table.shape[1]]
        copies.append(pltpu.make_async_copy(table, residual, save.at[count]))
        copies[-1].start()
    for copy in copies:
        copy.wait()


def finish(blocks, steps, result, others, systems, half, scale):
    rows = blocks[0].shape[0]
    count = len(blocks)
    hbm = pl.BlockSpec(memory_space=pltpu.HBM)
    vmem = pl.BlockSpec(memory_space=pltpu.VMEM)
    operands = list(blocks) + list(others) + ([] if result is None else [result])
    shapes = [jax.ShapeDtypeStruct((systems, 2 * half), jnp.float32)]
    if scale is not None:
        shapes.append(jax.ShapeDtypeStruct((SWEEPS, systems), jnp.float32))
    return pl.pallas_call(
        functools.partial(final_kernel, half, steps, scale),
        out_shape=shapes,
        in_specs=[vmem] * (count + len(others)) + ([] if result is None else [hbm]),
        out_specs=[hbm] * len(shapes),
        scratch_shapes=[pltpu.VMEM(shape.shape, jnp.float32) for shape in shapes[1:]]
        + [pltpu.SemaphoreType.DMA((count + 1,))],
        input_output_aliases={} if result is None else {len(operands) - 1: 0},
        compiler_params=pltpu.CompilerParams(vmem_limit_bytes=SMALL_LIMIT),
        cost_estimate=pl.CostEstimate(
            flops=count * rows * half, bytes_accessed=8 * count * rows * half, transcendentals=0
        ),
        name="finish",
    )(*operands)


def body(slice_starts, coupling):
    slices = lax.axis_size("tm")
    systems, cells = coupling.shape
    rows = systems // M
    half = cells // 2
    length = half + 2 * LANES
    count = slices * M
    flat, wide, core = (rows, length), (3, M, rows, length), (rows, half)
    small = (rows, LANES)

    def moved(value, target):
        pairs = [(i, target(i)) for i in range(slices)]
        return lax.ppermute(value, "tm", [(i, j) for i, j in pairs if 0 <= j < slices])

    def turned(value, target):
        return lax.ppermute(value, "tm", [(i, target(i) % slices) for i in range(slices)])

    mine, other = split(slice_starts[0], rows, length, 2)
    (near,) = split(coupling, rows, length, 1)
    partner = moved(other, lambda i: i ^ 1)
    crossed = moved(other, lambda i: (i ^ 1) + 2)
    straight = turned(mine, lambda i: i + 2)
    left_coupling, local, v_lo, slope_lo, u_hi, terms_hi, squares = call(
        pair_kernel, (near, mine, partner),
        [flat] * 4 + [wide, (M,) + flat, small], [flat] * 5, 300 * rows * length, LARGE_LIMIT,
    )
    (ending,) = call(
        start_kernel, (straight, crossed, v_lo, slope_lo, u_hi, terms_hi),
        [core], [], 50 * rows * length, SMALL_LIMIT,
    )
    ending = moved(ending, lambda i: i + 2)
    w_lo, w_hi, terms_lo, last_hi, squares = call(
        middle_kernel,
        (
            near, left_coupling, local, straight, crossed, v_lo, slope_lo, u_hi, terms_hi,
            squares,
        ),
        [wide, wide, (M,) + core, (M,) + core, (2,) + small], [flat] * 4 + [wide],
        600 * rows * length, LARGE_LIMIT,
    )
    last = (v_lo, ending, w_lo, w_hi, terms_lo, last_hi)
    even = call(
        functools.partial(late_kernel, 0), last, [core] * M, [],
        100 * rows * length, LARGE_LIMIT,
    )
    (payload,) = call(
        sums_kernel, last + (squares,), [(8, LANES)], [], 50 * rows * length,
        LARGE_LIMIT,
    )
    odd = call(
        functools.partial(late_kernel, 1), last, [(rows, half + LANES)] * M, [],
        100 * rows * length, LARGE_LIMIT,
    )
    for axis, step in rounds(slices):
        pairs = [(i, i ^ step) for i in range(lax.axis_size(axis))]
        payload = payload + lax.ppermute(payload, axis, pairs)
    odd = stamp(payload, odd)
    outs = [(odd if step % 2 else even)[step // 2] for step in range(2 * M)]
    blocks = list(outs)
    for step in home_order():
        pairs = [(i, i ^ step) for i in range(count)]
        blocks[step] = lax.ppermute(outs[step], ("tm", "node"), pairs)
    early = [0, 2, 4, 6, 7, 1]
    last = [5, 3]
    (result,) = finish([blocks[i] for i in early], early, None, [], systems, half, None)
    result, residual_log = finish(
        [blocks[i] for i in last], last, result, [blocks[7], blocks[1]], systems, half,
        slices * M * cells,
    )
    return (result[None, None], residual_log)


def home_order():
    return sorted(range(1, 2 * M), key=lambda step: (step % 2, -step))


def rounds(slices):
    found = [("node", 1)]
    step = 2
    while step < slices:
        found.append(("tm", step))
        step *= 2
    return found


def solution(mesh):
    placed = (P("tm", None, None), P())

    return jax.shard_map(
        body,
        mesh=mesh,
        in_specs=placed,
        out_specs=(P("tm", "node", None, None), P()),
        check_vma=False,
    )
```
